32 devices in a mesh: dp: 1, tp: 32 (over x, y, z, core).
Axes of the slice: x: 2, y: 2, z: 4, core: 2. Of those that a mesh axis runs over, the one named last changes fastest.
Arguments:
- x: bfloat16 [2048, 2048], P('dp')
- dy: bfloat16 [2048, 2048], P('dp')
- gate: bfloat16 [2048, 16384], P('dp', 'tp')
- up: bfloat16 [2048, 16384], P('dp', 'tp')
- w_gate: bfloat16 [2048, 16384], P(None, 'tp')
- w_up: bfloat16 [2048, 16384], P(None, 'tp')
- w_down: bfloat16 [16384, 2048], P('tp')
Outputs:
- output 1: bfloat16 [2048, 2048], P('dp')
- output 2: bfloat16 [2048, 16384], P('dp', 'tp')
- output 3: bfloat16 [2048, 16384], P('dp', 'tp')
- output 4: bfloat16 [16384, 2048], P(('dp', 'tp'))
All inputs are finite; a program needn't handle non-finite values.
Results may differ from the reference program's by a relative error of at most 0.012.
Values are sent between devices in bfloat16 or wider.
A program may use at most 2 GiB of HBM per device.

```python
import jax
import jax.numpy as jnp

ROWS = 2048
D = 2048
FF = 16384


def act(gate, up):
    return jax.nn.gelu(gate) * up


def setup_inputs(seed: int = 0, part: int = 0) -> dict:
    kx, ky, ka, kb, kg, ku, kd = jax.random.split(jax.random.key(seed), 7)
    kx, ky, ka, kb = (jax.random.fold_in(k, part) for k in (kx, ky, ka, kb))
    drawn = {
        "x": jax.random.normal(kx, (ROWS, D), jnp.float32),
        "dy": jax.random.normal(ky, (ROWS, D), jnp.float32),
        "gate": jax.random.normal(ka, (ROWS, FF), jnp.float32),
        "up": jax.random.normal(kb, (ROWS, FF), jnp.float32),
        "w_gate": jax.random.normal(kg, (D, FF), jnp.float32) * D**-0.5,
        "w_up": jax.random.normal(ku, (D, FF), jnp.float32) * D**-0.5,
        "w_down": jax.random.normal(kd, (FF, D), jnp.float32) * FF**-0.5,
    }
    return {k: v.astype(jnp.bfloat16) for k, v in drawn.items()}


def reference(x, dy, gate, up, w_gate, w_up, w_down):
    hidden, back = jax.vjp(act, gate.astype(jnp.float32), up.astype(jnp.float32))
    d_hidden = jnp.dot(dy, w_down.T, preferred_element_type=jnp.float32)
    d_gate, d_up = (g.astype(jnp.bfloat16) for g in back(d_hidden))
    dx = jnp.dot(d_gate, w_gate.T, preferred_element_type=jnp.float32) + jnp.dot(d_up, w_up.T, preferred_element_type=jnp.float32)
    dw_gate = jnp.dot(x.T, d_gate, preferred_element_type=jnp.float32)
    dw_up = jnp.dot(x.T, d_up, preferred_element_type=jnp.float32)
    dw_down = jnp.dot(hidden.astype(jnp.bfloat16).T, dy, preferred_element_type=jnp.float32)
    return tuple(g.astype(jnp.bfloat16) for g in (dx, dw_gate, dw_up, dw_down))
```

```python
import functools

import jax
import jax.numpy as jnp
from jax import lax
from jax.experimental import pallas as pl
from jax.experimental.pallas import tpu as pltpu
from jax.sharding import PartitionSpec as P

MESH = pl.DeviceIdType.MESH
BF = jnp.bfloat16
F32 = jnp.float32

ROWS = 2048
D = 2048
F = 512
R = 256
K = ROWS // R
HALF = D // 2
QC = HALF // 2
NB = 8
CB = D // NB

OFFS = {1: 1, 2: 3, 3: 5, 4: 7, 5: 9, 6: 11, 7: 13, 8: 15, 9: 17, 10: 18}
STEPS = K + OFFS[10]


def act(gate, up):
    return jax.nn.gelu(gate) * up


def dot_nt(a, b):
    return lax.dot_general(a, b, (((1,), (1,)), ((), ())), preferred_element_type=F32)


def dot_tn(a, b):
    return lax.dot_general(a, b, (((0,), (0,)), ((), ())), preferred_element_type=F32)


def kernel(
    x_hbm, dy_hbm, gate_hbm, up_hbm, wg_hbm, wu_hbm, wd_hbm,
    dx, dwg, dwu, dwd,
    wd, wcat, gu, hid_t, dyr, xc, dyc, own, cs, cr,
    s1, r1, s2, r2, s3, r3, s4, r4,
    ssem, rsem, wsem, gsem, dsem, bsem,
):
    me = lax.axis_index("tp")
    c = lax.rem(me, 2)
    zl = lax.rem(me // 2, 2)
    zh = lax.rem(me // 4, 2)
    y = lax.rem(me // 8, 2)
    x = me // 16
    pc = me + 1 - 2 * c
    pz1 = me + 2 - 4 * zl
    pz2 = me + 4 - 8 * zh
    py = me + 8 - 16 * y
    px = me + 16 - 32 * x

    def row_copy(k, slot):
        return pltpu.make_async_copy(dy_hbm.at[pl.ds(k * R, R)], dyr.at[slot], dsem.at[slot])

    def gate_copies(k):
        rows = pl.ds(k * R, R)
        return (
            pltpu.make_async_copy(gate_hbm.at[rows], gu.at[rows, pl.ds(0, F)], gsem.at[0, k]),
            pltpu.make_async_copy(up_hbm.at[rows], gu.at[rows, pl.ds(F, F)], gsem.at[1, k]),
        )

    w_copies = (
        pltpu.make_async_copy(wd_hbm, wd, wsem.at[0]),
        pltpu.make_async_copy(wg_hbm, wcat.at[:, pl.ds(0, F)], wsem.at[1]),
        pltpu.make_async_copy(wu_hbm, wcat.at[:, pl.ds(F, F)], wsem.at[2]),
    )

    def block_copy(which, j, slot):
        columns = pl.ds(j * CB, CB)
        src, dst = ((x_hbm, xc), (dy_hbm, dyc))[which]
        return pltpu.make_async_copy(src.at[:, columns], dst.at[slot], bsem.at[which, slot])

    row_copy(0, 0).start()
    w_copies[0].start()
    for cp in gate_copies(0):
        cp.start()
    w_copies[1].start()
    w_copies[2].start()
    row_copy(1, 1).start()
    for k in range(1, K):
        for cp in gate_copies(k):
            cp.start()
    for which in range(2):
        block_copy(which, 0, 0).start()

    barrier = pltpu.get_barrier_semaphore()
    partners = (pc, pz1, pz2, py, px)
    for p in partners:
        pl.semaphore_signal(barrier, inc=1, device_id=(0, p), device_id_type=MESH)
    pl.semaphore_wait(barrier, len(partners))

    def remote(src, dst, stage, color, k, p):
        return pltpu.make_async_remote_copy(
            src_ref=src, dst_ref=dst,
            send_sem=ssem.at[stage, color, k], recv_sem=rsem.at[stage, color, k],
            device_id=(0, p), device_id_type=MESH,
        )

    def m16(v):
        return pl.multiple_of(v, 16)

    own_col = pl.multiple_of(c * HALF, HALF)
    other_col = pl.multiple_of((1 - c) * HALF, HALF)

    BITS = ((x, y, px, py), (y, x, py, px))

    def core_copy(k):
        rows = pl.ds(pl.multiple_of(k * R, R), R)
        return remote(cs.at[rows], cr.at[rows], 0, 0, k, pc)

    def level_copy(level, e, k):
        s, r, p = (
            (s1, r1, BITS[e][2]), (s2, r2, pz1), (s3, r3, BITS[e][3]), (s4, r4, pz2),
        )[level - 1]
        n = R >> level
        rows = pl.ds(m16(k * n), n)
        return remote(s.at[e, rows], r.at[e, rows], level, e, k, p)

    def kept(level, e):
        b1, b3 = BITS[e][:2]
        bits = (b1, zl, b3, zh)
        return sum((bits[i] * (R >> (i + 1)) for i in range(level)), 0)

    def gather_copy(level, e, k, mine):
        p = (BITS[e][2], pz1, BITS[e][3], pz2)[level - 1]
        n = R >> level
        off = kept(level, e)
        if not mine:
            b = (BITS[e][0], zl, BITS[e][1], zh)[level - 1]
            off = off + (1 - 2 * b) * n
        view = dx.at[pl.ds(m16(k * R + off), n), pl.ds(pl.multiple_of(own_col + e * QC, QC), QC)]
        return remote(view, view, 9 - level, e, k, p)

    def out_copy(k, mine):
        view = dx.at[pl.ds(pl.multiple_of(k * R, R), R), pl.ds(own_col if mine else other_col, HALF)]
        return remote(view, view, 9, 0, k, pc)

    def total(level, e, k, off, n):
        cols = pl.ds(e * QC, QC)
        rows = pl.ds(m16(k * R + off), n)
        acc = own[rows, cols] + cr[rows, cols].astype(F32)
        recv = (r1, r2, r3, r4)
        for i in range(level):
            m = R >> (i + 1)
            local = off - kept(i + 1, e)
            acc = acc + recv[i][e, pl.ds(m16(k * m + local), n), :].astype(F32)
        return acc

    def reduce_stage(level, k):
        if level == 1:
            core_copy(k).wait_recv()
        for e in range(2):
            if level > 1:
                level_copy(level - 1, e, k).wait_recv()
            n = R >> level
            b = (BITS[e][0], zl, BITS[e][1], zh)[level - 1]
            off = kept(level - 1, e) + (1 - b) * n
            stage = (s1, s2, s3, s4)[level - 1]
            stage[e, pl.ds(m16(k * n), n), :] = total(level - 1, e, k, off, n).astype(BF)
            level_copy(level, e, k).start()

    def finish_stage(k):
        n = R >> 4
        for e in range(2):
            level_copy(4, e, k).wait_recv()
            off = kept(4, e)
            cols = pl.ds(pl.multiple_of(own_col + e * QC, QC), QC)
            dx[pl.ds(m16(k * R + off), n), cols] = total(4, e, k, off, n).astype(BF)
            gather_copy(4, e, k, True).start()

    def gather_stage(level, k):
        for e in range(2):
            gather_copy(level + 1, e, k, False).wait_recv()
            gather_copy(level, e, k, True).start()

    def last_stage(k):
        for e in range(2):
            gather_copy(1, e, k, False).wait_recv()
        out_copy(k, True).start()

    STAGES = {
        1: lambda k: reduce_stage(1, k),
        2: lambda k: reduce_stage(2, k),
        3: lambda k: reduce_stage(3, k),
        4: lambda k: reduce_stage(4, k),
        5: finish_stage,
        6: lambda k: gather_stage(3, k),
        7: lambda k: gather_stage(2, k),
        8: lambda k: gather_stage(1, k),
        9: last_stage,
        10: lambda k: out_copy(k, False).wait_recv(),
    }

    def compute_terms(k):
        slot = lax.rem(k, 2)
        r0 = pl.multiple_of(k * R, R)
        rows = pl.ds(r0, R)
        row_copy(k, slot).wait()
        for cp in gate_copies(k):
            cp.wait()

        @pl.when(k == 0)
        def _():
            w_copies[0].wait()

        for h in range(2):
            hc = pl.ds(h * (F // 2), F // 2)
            d_hidden = dot_nt(dyr[slot], wd[hc, :])
            g = gu[rows, pl.ds(h * (F // 2), F // 2)].astype(F32)
            u = gu[rows, pl.ds(F + h * (F // 2), F // 2)].astype(F32)
            hidden, back = jax.vjp(act, g, u)
            d_gate, d_up = back(d_hidden)
            gu[rows, pl.ds(h * (F // 2), F // 2)] = d_gate.astype(BF)
            gu[rows, pl.ds(F + h * (F // 2), F // 2)] = d_up.astype(BF)
            hid_t[hc, rows] = hidden.astype(BF).T

        @pl.when(k + 2 < K)
        def _():
            row_copy(k + 2, slot).start()

        @pl.when(k == 0)
        def _():
            w_copies[1].wait()
            w_copies[2].wait()

        d_cat = gu[rows, :]
        for n in range(2):
            cs[rows, pl.ds(n * QC, QC)] = dot_nt(d_cat, wcat[pl.ds(pl.multiple_of(other_col + n * QC, QC), QC), :]).astype(BF)
        core_copy(k).start()
        for n in range(2):
            own[rows, pl.ds(n * QC, QC)] = dot_nt(d_cat, wcat[pl.ds(pl.multiple_of(own_col + n * QC, QC), QC), :])

    def compute_weights(j, part):
        slot = lax.rem(j, 2)
        if part == 0:
            @pl.when(j + 1 < NB)
            def _():
                for which in range(2):
                    block_copy(which, j + 1, 1 - slot).start()

            block_copy(0, j, slot).wait()
            rows = pl.ds(pl.multiple_of(j * CB, CB), CB)
            dw = dot_tn(xc[slot], gu[...])
            dwg[rows, :] = dw[:, :F].astype(BF)
            dwu[rows, :] = dw[:, F:].astype(BF)
        else:
            block_copy(1, j, slot).wait()
            cols = pl.ds(pl.multiple_of(j * CB, CB), CB)
            dwd[:, cols] = jnp.dot(hid_t[...], dyc[slot], preferred_element_type=F32).astype(BF)

    def step(t, carry):
        def at(stage):
            k = t - OFFS[stage]

            @pl.when((k >= 0) & (k < K))
            def _():
                STAGES[stage](k)

        @pl.when(t < K)
        def _():
            compute_terms(t)

        for stage in (10, 9, 8, 7, 6):
            at(stage)

        @pl.when((t >= K) & (t < K + NB))
        def _():
            compute_weights(t - K, 0)

        for stage in (5, 4, 3, 2, 1):
            at(stage)

        @pl.when((t >= K) & (t < K + NB))
        def _():
            compute_weights(t - K, 1)

        return carry

    lax.fori_loop(0, STEPS, step, 0)

    def drain(k, carry):
        core_copy(k).wait_send()
        for e in range(2):
            for level in range(1, 5):
                level_copy(level, e, k).wait_send()
                gather_copy(level, e, k, True).wait_send()
        out_copy(k, True).wait_send()
        return carry

    lax.fori_loop(0, K, drain, 0)


def solution(mesh):
    def step(x, dy, gate, up, w_gate, w_up, w_down):
        def out(*shape):
            return pltpu.VMEM(shape, BF)

        def buf(*shape, dtype=BF):
            return pltpu.VMEM(shape, dtype)

        scratch = [
            buf(F, D), buf(D, 2 * F), buf(ROWS, 2 * F), buf(F, ROWS),
            buf(2, R, D), buf(2, ROWS, CB), buf(2, ROWS, CB),
            buf(ROWS, HALF, dtype=F32), buf(ROWS, HALF), buf(ROWS, HALF),
        ]
        for level in range(1, 5):
            scratch += [buf(2, ROWS >> level, QC), buf(2, ROWS >> level, QC)]
        sem = pltpu.SemaphoreType.DMA
        scratch += [sem((10, 2, K)), sem((10, 2, K)), sem((3,)), sem((2, K)), sem((2,)), sem((2, 2))]
        return tuple(
            pl.pallas_call(
                kernel,
                name="backward",
                out_shape=[out(ROWS, D), out(D, F), out(D, F), out(F, D)],
                in_specs=[pl.BlockSpec(memory_space=pl.ANY)] * 7,
                out_specs=[pl.BlockSpec(memory_space=pltpu.VMEM)] * 4,
                scratch_shapes=scratch,
                compiler_params=pltpu.CompilerParams(
                    collective_id=0, has_side_effects=True, vmem_limit_bytes=49 << 20
                ),
            )(x, dy, gate, up, w_gate, w_up, w_down)
        )

    tokens, columns, rows = P("dp", None), P(None, "tp"), P("tp", None)
    return jax.shard_map(
        step,
        mesh=mesh,
        in_specs=(tokens, tokens, P("dp", "tp"), P("dp", "tp"), columns, columns, rows),
        out_specs=(tokens, P("dp", "tp"), P("dp", "tp"), P(("dp", "tp"), None)),
        check_vma=False,
    )
```

```python
import functools

import jax
import jax.numpy as jnp
from jax import lax
from jax.experimental import pallas as pl
from jax.experimental.pallas import tpu as pltpu
from jax.sharding import PartitionSpec as P

MESH = pl.DeviceIdType.MESH
BF = jnp.bfloat16
F32 = jnp.float32

ROWS = 2048
D = 2048
F = 512
RC = 256
KC = ROWS // RC
K = 16
R = ROWS // K
PER = K // KC
HALF = D // 2
QC = HALF // 2
NB = 8
CB = D // NB

DELTAS = (2, 3, 3, 2, 3, 3, 6, 3, 9, 3)
OFFS = {i + 1: sum(DELTAS[: i + 1]) for i in range(10)}
STEPS = K + max(OFFS[10], 3 * NB)
NSLICE = 3 * NB


def block_sizes():
    sizes = [(R, QC)]
    for _ in range(4):
        n, m = sizes[-1]
        sizes.append((n // 2, m) if n > 16 else (n, m // 2))
    return sizes


SZ = block_sizes()


def act(gate, up):
    return jax.nn.gelu(gate) * up


def dot_nt(a, b):
    return lax.dot_general(a, b, (((1,), (1,)), ((), ())), preferred_element_type=F32)


def dot_tn(a, b):
    return lax.dot_general(a, b, (((0,), (0,)), ((), ())), preferred_element_type=F32)


def kernel(
    x_hbm, dy_hbm, gate_hbm, up_hbm, wg_hbm, wu_hbm, wd_hbm,
    dx, dwg, dwu, dwd,
    wd, wcat, gu, hid_t, dyr, xc, dyc, own, cs, cr,
    s1, r1, s2, r2, s3, r3, s4, r4,
    ssem, rsem, wsem, gsem, dsem, bsem,
):
    me = lax.axis_index("tp")
    c = lax.rem(me, 2)
    zl = lax.rem(me // 2, 2)
    zh = lax.rem(me // 4, 2)
    y = lax.rem(me // 8, 2)
    x = me // 16
    pc = me + 1 - 2 * c
    pz1 = me + 2 - 4 * zl
    pz2 = me + 4 - 8 * zh
    py = me + 8 - 16 * y
    px = me + 16 - 32 * x

    def row_copy(k, slot):
        return pltpu.make_async_copy(dy_hbm.at[pl.ds(k * RC, RC)], dyr.at[slot], dsem.at[slot])

    def gate_copies(k):
        rows = pl.ds(k * RC, RC)
        return (
            pltpu.make_async_copy(gate_hbm.at[rows], gu.at[rows, pl.ds(0, F)], gsem.at[0, k]),
            pltpu.make_async_copy(up_hbm.at[rows], gu.at[rows, pl.ds(F, F)], gsem.at[1, k]),
        )

    w_copies = (
        pltpu.make_async_copy(wd_hbm, wd, wsem.at[0]),
        pltpu.make_async_copy(wg_hbm, wcat.at[:, pl.ds(0, F)], wsem.at[1]),
        pltpu.make_async_copy(wu_hbm, wcat.at[:, pl.ds(F, F)], wsem.at[2]),
    )

    def block_copy(which, j, slot):
        columns = pl.ds(j * CB, CB)
        src, dst = ((x_hbm, xc), (dy_hbm, dyc))[which]
        return pltpu.make_async_copy(src.at[:, columns], dst.at[slot], bsem.at[which, slot])

    row_copy(0, 0).start()
    w_copies[0].start()
    for cp in gate_copies(0):
        cp.start()
    w_copies[1].start()
    w_copies[2].start()

    barrier = pltpu.get_barrier_semaphore()
    partners = (pc, pz1, pz2, py, px)
    for p in partners:
        pl.semaphore_signal(barrier, inc=1, device_id=(0, p), device_id_type=MESH)

    def remote(src, dst, stage, color, k, p):
        return pltpu.make_async_remote_copy(
            src_ref=src, dst_ref=dst,
            send_sem=ssem.at[stage, color], recv_sem=rsem.at[stage, color, k],
            device_id=(0, p), device_id_type=MESH,
        )

    def m16(v):
        return pl.multiple_of(v, 16)

    own_col = pl.multiple_of(c * HALF, HALF)
    other_col = pl.multiple_of((1 - c) * HALF, HALF)

    BITS = ((x, y, px, py), (y, x, py, px))

    def core_copy(k):
        rows = pl.ds(pl.multiple_of(k * R, R), R)
        return remote(cs.at[rows], cr.at[rows], 0, 0, k, pc)

    def m128(v):
        return v if isinstance(v, int) else pl.multiple_of(v, 128)

    def level_copy(level, e, k):
        s, r, p = (
            (s1, r1, BITS[e][2]), (s2, r2, pz1), (s3, r3, BITS[e][3]), (s4, r4, pz2),
        )[level - 1]
        n = SZ[level][0]
        rows = pl.ds(m16(k * n), n)
        return remote(s.at[e, rows], r.at[e, rows], level, e, k, p)

    def offset(level, e, flip=False):
        b1, b3 = BITS[e][:2]
        bits = (b1, zl, b3, zh)
        row = col = 0
        for i in range(level):
            b = bits[i]
            if flip and i == level - 1:
                b = 1 - b
            if SZ[i + 1][0] < SZ[i][0]:
                row = row + b * SZ[i + 1][0]
            else:
                col = col + b * SZ[i + 1][1]
        return row, col

    def gather_copy(level, e, k, mine):
        p = (BITS[e][2], pz1, BITS[e][3], pz2)[level - 1]
        n, m = SZ[level]
        row, col = offset(level, e, not mine)
        view = dx.at[pl.ds(m16(k * R + row), n), pl.ds(pl.multiple_of(own_col + e * QC + col, 128), m)]
        return remote(view, view, 9 - level, e, k, p)

    def out_copy(k, mine):
        view = dx.at[pl.ds(pl.multiple_of(k * R, R), R), pl.ds(own_col if mine else other_col, HALF)]
        return remote(view, view, 9, 0, k, pc)

    def total(level, e, k, off, size):
        (row, col), (n, m) = off, size
        rows, cols = pl.ds(m16(k * R + row), n), pl.ds(m128(e * QC + col), m)
        acc = own[rows, cols] + cr[rows, cols].astype(F32)
        recv = (r1, r2, r3, r4)
        for i in range(level):
            krow, kcol = offset(i + 1, e)
            rows = pl.ds(m16(k * SZ[i + 1][0] + row - krow), n)
            acc = acc + recv[i][e, rows, pl.ds(m128(col - kcol), m)].astype(F32)
        return acc

    def reduce_stage(level, k):
        if level == 1:
            core_copy(k).wait_recv()
        for e in range(2):
            if level > 1:
                level_copy(level - 1, e, k).wait_recv()
            n = SZ[level][0]
            stage = (s1, s2, s3, s4)[level - 1]
            stage[e, pl.ds(m16(k * n), n), :] = total(level - 1, e, k, offset(level, e, True), SZ[level]).astype(BF)
            level_copy(level, e, k).start()

    def finish_stage(k):
        n, m = SZ[4]
        for e in range(2):
            level_copy(4, e, k).wait_recv()
            row, col = offset(4, e)
            cols = pl.ds(pl.multiple_of(own_col + e * QC + col, 128), m)
            dx[pl.ds(m16(k * R + row), n), cols] = total(4, e, k, (row, col), (n, m)).astype(BF)
            gather_copy(4, e, k, True).start()

    def gather_stage(level, k):
        for e in range(2):
            gather_copy(level + 1, e, k, False).wait_recv()
            gather_copy(level, e, k, True).start()

    def last_stage(k):
        for e in range(2):
            gather_copy(1, e, k, False).wait_recv()
        out_copy(k, True).start()

    STAGES = {
        1: lambda k: reduce_stage(1, k),
        2: lambda k: reduce_stage(2, k),
        3: lambda k: reduce_stage(3, k),
        4: lambda k: reduce_stage(4, k),
        5: finish_stage,
        6: lambda k: gather_stage(3, k),
        7: lambda k: gather_stage(2, k),
        8: lambda k: gather_stage(1, k),
        9: last_stage,
        10: lambda k: out_copy(k, False).wait_recv(),
    }

    def compute_gates(k):
        slot = lax.rem(k, 2)
        rows = pl.ds(pl.multiple_of(k * RC, RC), RC)
        row_copy(k, slot).wait()
        for cp in gate_copies(k):
            cp.wait()

        for h in range(2):
            hc = pl.ds(h * (F // 2), F // 2)
            d_hidden = dot_nt(dyr[slot], wd[hc, :])
            g = gu[rows, pl.ds(h * (F // 2), F // 2)].astype(F32)
            u = gu[rows, pl.ds(F + h * (F // 2), F // 2)].astype(F32)
            hidden, back = jax.vjp(act, g, u)
            d_gate, d_up = back(d_hidden)
            gu[rows, pl.ds(h * (F // 2), F // 2)] = d_gate.astype(BF)
            gu[rows, pl.ds(F + h * (F // 2), F // 2)] = d_up.astype(BF)
            hid_t[hc, rows] = hidden.astype(BF).T

        @pl.when(k + 2 < KC)
        def _():
            row_copy(k + 2, slot).start()
            for cp in gate_copies(k + 2):
                cp.start()

    def compute_terms(k, part):
        rows = pl.ds(pl.multiple_of(k * RC, RC), RC)
        d_cat = gu[rows, :]
        if part == 0:
            for n in range(2):
                at = pl.ds(pl.multiple_of(other_col + n * QC, QC), QC)
                cs[rows, pl.ds(n * QC, QC)] = dot_nt(d_cat, wcat[at, :]).astype(BF)
        else:
            n = part - 1
            at = pl.ds(pl.multiple_of(own_col + n * QC, QC), QC)
            own[rows, pl.ds(n * QC, QC)] = dot_nt(d_cat, wcat[at, :])

    def start_core(k):
        for i in range(PER):
            core_copy(k * PER + i).start()

    def compute_weights(j, part):
        slot = lax.rem(j, 2)
        if part == 0:
            @pl.when(j + 1 < NB)
            def _():
                for which in range(2):
                    block_copy(which, j + 1, 1 - slot).start()

            block_copy(0, j, slot).wait()
        if part < 2:
            rows = pl.ds(pl.multiple_of(j * CB, CB), CB)
            (dwg, dwu)[part][rows, :] = dot_tn(xc[slot], gu[:, pl.ds(part * F, F)]).astype(BF)
        else:
            block_copy(1, j, slot).wait()
            cols = pl.ds(pl.multiple_of(j * CB, CB), CB)
            dwd[:, cols] = jnp.dot(hid_t[...], dyc[slot], preferred_element_type=F32).astype(BF)

    def when(condition, f, *args):
        @pl.when(condition)
        def _():
            f(*args)

    def step(t, carry):
        k, part = t // PER, lax.rem(t, PER)
        first = t < K
        def send_terms(k):
            compute_terms(k, 0)
            start_core(k)

        slices = [compute_gates, send_terms] + [functools.partial(compute_terms, part=i) for i in (1, 2)]
        for i in range(PER):
            def run(k, i=i):
                for f in slices[i * 4 // PER : (i + 1) * 4 // PER]:
                    f(k)

            when(first & (part == i) & ((k > 0) if i < max(1, PER // 2) else True), run, k)

        @pl.when(t == K - 2 * PER)
        def _():
            for which in range(2):
                block_copy(which, 0, 0).start()

        v = t - K
        j, part = v // 3, lax.rem(v, 3)
        second = (v >= 0) & (v < NSLICE)
        for i in range(3):
            when(second & (part == i), compute_weights, j, i)

        for stage in range(10, 0, -1):
            q = t - OFFS[stage]
            when((q >= 0) & (q < K), STAGES[stage], q)

        return carry

    w_copies[0].wait()
    compute_gates(0)
    row_copy(1, 1).start()
    for cp in gate_copies(1):
        cp.start()
    w_copies[1].wait()
    w_copies[2].wait()
    compute_terms(0, 0)
    pl.semaphore_wait(barrier, len(partners))
    start_core(0)

    lax.fori_loop(0, STEPS, step, 0)

    def sent(ref, stage, color):
        pltpu.make_async_copy(ref, ref, ssem.at[stage, color]).wait()

    sent(cs, 0, 0)
    sent(cs, 9, 0)
    for e in range(2):
        for level, ref in enumerate((s1, s2, s3, s4), 1):
            sent(ref.at[e], level, e)
            sent(ref.at[e], 9 - level, e)


def write_out(*refs):
    sources, targets, sem = refs[:4], refs[4:8], refs[8]
    copies = [pltpu.make_async_copy(s, t, sem.at[i]) for i, (s, t) in enumerate(zip(sources, targets))]
    for cp in copies:
        cp.start()
    for cp in copies:
        cp.wait()


def solution(mesh):
    def step(x, dy, gate, up, w_gate, w_up, w_down):
        def out(*shape):
            return pltpu.VMEM(shape, BF)

        def buf(*shape, dtype=BF):
            return pltpu.VMEM(shape, dtype)

        scratch = [
            buf(F, D), buf(D, 2 * F), buf(ROWS, 2 * F), buf(F, ROWS),
            buf(2, RC, D), buf(2, ROWS, CB), buf(2, ROWS, CB),
            buf(ROWS, HALF, dtype=F32), buf(ROWS, HALF), buf(ROWS, HALF),
        ]
        for n, m in SZ[1:]:
            scratch += [buf(2, K * n, m), buf(2, K * n, m)]
        sem = pltpu.SemaphoreType.DMA
        scratch += [sem((10, 2)), sem((10, 2, K)), sem((3,)), sem((2, KC)), sem((2,)), sem((2, 2))]
        held = (
            pl.pallas_call(
                kernel,
                name="backward",
                out_shape=[out(ROWS, D), out(D, F), out(D, F), out(F, D)],
                in_specs=[pl.BlockSpec(memory_space=pl.ANY)] * 7,
                out_specs=[pl.BlockSpec(memory_space=pltpu.VMEM)] * 4,
                scratch_shapes=scratch,
                compiler_params=pltpu.CompilerParams(
                    collective_id=0, has_side_effects=True, vmem_limit_bytes=49 << 20
                ),
            )(x, dy, gate, up, w_gate, w_up, w_down)
        )
        return tuple(
            pl.pallas_call(
                write_out,
                name="write_out",
                out_shape=[jax.ShapeDtypeStruct(v.shape, BF) for v in held],
                in_specs=[pl.BlockSpec(memory_space=pltpu.VMEM)] * 4,
                out_specs=[pl.BlockSpec(memory_space=pl.ANY)] * 4,
                scratch_shapes=[sem((4,))],
                compiler_params=pltpu.CompilerParams(vmem_limit_bytes=1 << 20),
            )(*(pltpu.with_memory_space_constraint(v, pltpu.VMEM) for v in held))
        )

    tokens, columns, rows = P("dp", None), P(None, "tp"), P("tp", None)
    return jax.shard_map(
        step,
        mesh=mesh,
        in_specs=(tokens, tokens, P("dp", "tp"), P("dp", "tp"), columns, columns, rows),
        out_specs=(tokens, P("dp", "tp"), P("dp", "tp"), P(("dp", "tp"), None)),
        check_vma=False,
    )
```

```python
import functools

import jax
import jax.numpy as jnp
from jax import lax
from jax.experimental import pallas as pl
from jax.experimental.pallas import tpu as pltpu
from jax.sharding import PartitionSpec as P

MESH = pl.DeviceIdType.MESH
BF = jnp.bfloat16
F32 = jnp.float32

ROWS = 2048
D = 2048
F = 512
RC = 256
KC = ROWS // RC
K = 16
R = ROWS // K
PER = K // KC
HALF = D // 2
QC = HALF // 2
NB = 8
CB = D // NB

DELTAS = (1, 3, 3, 3, 3, 3, 3, 3, 4, 2)
OFFS = {i + 1: sum(DELTAS[: i + 1]) for i in range(10)}
ST = 4
MID = K + ST * NB // 2
STEPS = max(MID, K + OFFS[10])
SLOTS = tuple(min(K, 2 * d + (4 if i == 0 else 1)) for i, d in enumerate(DELTAS))
BASE = tuple(sum(SLOTS[:i]) for i in range(11))


def block_sizes():
    sizes = [(R, QC)]
    for _ in range(4):
        n, m = sizes[-1]
        sizes.append((n // 2, m) if n > 16 else (n, m // 2))
    return sizes


SZ = block_sizes()


C0 = 0.7978845608028654
C1 = 0.044715


def gelu_and_slope(g):
    square = g * g
    th = jnp.tanh(C0 * (g + C1 * (square * g)))
    cdf = 0.5 * (1.0 + th)
    slope = cdf + (g * (0.5 * (1.0 - th * th))) * (C0 * (1.0 + (3.0 * C1) * square))
    return g * cdf, slope


def dot_nt(a, b):
    return lax.dot_general(a, b, (((1,), (1,)), ((), ())), preferred_element_type=F32)


def dot_tn(a, b):
    return lax.dot_general(a, b, (((0,), (0,)), ((), ())), preferred_element_type=F32)


def kernel(
    x_hbm, dy_hbm, gate_hbm, up_hbm, wg_hbm, wu_hbm, wd_hbm,
    dx, dwg, dwu, dwd,
    wd, wcat, gu, gelu, slope, hid_t, dyr, xc, dyc, own, cs, cr,
    s1, r1, s2, r2, s3, r3, s4, r4,
    ssem, rsem, wsem, gsem, dsem, bsem,
):
    me = lax.axis_index("tp")
    c = lax.rem(me, 2)
    zl = lax.rem(me // 2, 2)
    zh = lax.rem(me // 4, 2)
    y = lax.rem(me // 8, 2)
    x = me // 16
    pc = me + 1 - 2 * c
    pz1 = me + 2 - 4 * zl
    pz2 = me + 4 - 8 * zh
    py = me + 8 - 16 * y
    px = me + 16 - 32 * x

    def row_copy(k, slot):
        return pltpu.make_async_copy(dy_hbm.at[pl.ds(k * RC, RC)], dyr.at[slot], dsem.at[slot])

    def gate_copies(k):
        rows = pl.ds(k * RC, RC)
        return (
            pltpu.make_async_copy(gate_hbm.at[rows], gu.at[rows, pl.ds(0, F)], gsem.at[0, k]),
            pltpu.make_async_copy(up_hbm.at[rows], gu.at[rows, pl.ds(F, F)], gsem.at[1, k]),
        )

    w_copies = (
        pltpu.make_async_copy(wd_hbm, wd, wsem.at[0]),
        pltpu.make_async_copy(wg_hbm, wcat.at[:, pl.ds(0, F)], wsem.at[1]),
        pltpu.make_async_copy(wu_hbm, wcat.at[:, pl.ds(F, F)], wsem.at[2]),
    )

    def block_copy(which, j, slot):
        columns = pl.ds(j * CB, CB)
        src, dst = ((x_hbm, xc), (dy_hbm, dyc))[which]
        return pltpu.make_async_copy(src.at[:, columns], dst.at[slot], bsem.at[which, slot])

    for cp in gate_copies(0):
        cp.start()
    row_copy(0, 0).start()
    w_copies[0].start()

    barrier = pltpu.get_barrier_semaphore()
    partners = (pc, pz1, pz2, py, px)
    for p in partners:
        pl.semaphore_signal(barrier, inc=1, device_id=(0, p), device_id_type=MESH)

    def remote(src, dst, stage, color, k, p):
        return pltpu.make_async_remote_copy(
            src_ref=src, dst_ref=dst,
            send_sem=ssem.at[stage, color], recv_sem=rsem.at[slot(stage, k)],
            device_id=(0, p), device_id_type=MESH,
        )

    def m16(v):
        return pl.multiple_of(v, 16)

    own_col = pl.multiple_of(c * HALF, HALF)
    other_col = pl.multiple_of((1 - c) * HALF, HALF)

    def route(e, k):
        a, b, pa, pb = ((x, y, px, py), (y, x, py, px))[e]
        return (a, zl, b, zh), (pa, pz1, pb, pz2)

    def slot(stage, k):
        return BASE[stage] + lax.rem(k, SLOTS[stage])

    def core_copy(k):
        rows = pl.ds(pl.multiple_of(k * R, R), R)
        return remote(cs.at[rows], cr.at[rows], 0, 0, k, pc)

    def m128(v):
        return v if isinstance(v, int) else pl.multiple_of(v, 128)

    def level_copy(level, e, k):
        s, r = ((s1, r1), (s2, r2), (s3, r3), (s4, r4))[level - 1]
        p = route(e, k)[1][level - 1]
        n = SZ[level][0]
        rows = pl.ds(m16(k * n), n)
        return remote(s.at[e, rows], r.at[e, rows], level, e, k, p)

    def received(stage, k):
        level = stage if stage < 5 else 9 - stage
        if level == 0:
            ref = cr.at[pl.ds(m16(k * R), R)]
        else:
            n = SZ[level][0]
            ref = (r1, r2, r3, r4)[level - 1].at[:, pl.ds(m16(k * n), n)]
        pltpu.make_async_copy(ref, ref, rsem.at[slot(stage, k)]).wait()

    def offset(level, e, k, flip=False):
        bits = route(e, k)[0]
        row = col = 0
        for i in range(level):
            b = bits[i]
            if flip and i == level - 1:
                b = 1 - b
            if SZ[i + 1][0] < SZ[i][0]:
                row = row + b * SZ[i + 1][0]
            else:
                col = col + b * SZ[i + 1][1]
        return row, col

    def gather_copy(level, e, k):
        p = route(e, k)[1][level - 1]
        n, m = SZ[level]
        row, col = offset(level, e, k)
        view = dx.at[pl.ds(m16(k * R + row), n), pl.ds(pl.multiple_of(own_col + e * QC + col, 128), m)]
        return remote(view, view, 9 - level, e, k, p)

    def out_copy(k):
        view = dx.at[pl.ds(pl.multiple_of(k * R, R), R), pl.ds(own_col, HALF)]
        return remote(view, view, 9, 0, k, pc)

    def total(level, e, k, off, size):
        (row, col), (n, m) = off, size
        rows, cols = pl.ds(m16(k * R + row), n), pl.ds(m128(e * QC + col), m)
        acc = own[rows, cols] + cr[rows, cols].astype(F32)
        recv = (r1, r2, r3, r4)
        for i in range(level):
            krow, kcol = offset(i + 1, e, k)
            rows = pl.ds(m16(k * SZ[i + 1][0] + row - krow), n)
            acc = acc + recv[i][e, rows, pl.ds(m128(col - kcol), m)].astype(F32)
        return acc

    def reduce_stage(level, k):
        received(level - 1, k)
        for e in range(2):
            n = SZ[level][0]
            stage = (s1, s2, s3, s4)[level - 1]
            stage[e, pl.ds(m16(k * n), n), :] = total(level - 1, e, k, offset(level, e, k, True), SZ[level]).astype(BF)
            level_copy(level, e, k).start()

    def finish_stage(k):
        n, m = SZ[4]
        received(4, k)
        for e in range(2):
            row, col = offset(4, e, k)
            cols = pl.ds(pl.multiple_of(own_col + e * QC + col, 128), m)
            dx[pl.ds(m16(k * R + row), n), cols] = total(4, e, k, (row, col), (n, m)).astype(BF)
            gather_copy(4, e, k).start()

    def gather_stage(level, k):
        received(8 - level, k)
        for e in range(2):
            gather_copy(level, e, k).start()

    def last_stage(k):
        received(8, k)
        out_copy(k).start()

    STAGES = {
        1: lambda k: reduce_stage(1, k),
        2: lambda k: reduce_stage(2, k),
        3: lambda k: reduce_stage(3, k),
        4: lambda k: reduce_stage(4, k),
        5: finish_stage,
        6: lambda k: gather_stage(3, k),
        7: lambda k: gather_stage(2, k),
        8: lambda k: gather_stage(1, k),
        9: last_stage,
        10: lambda k: received(9, k),
    }

    def prepare(k, then=None):
        rows = pl.ds(pl.multiple_of(k * RC, RC), RC)
        for cp in gate_copies(k):
            cp.wait()
        if then is not None:
            then()
        value, slope[...] = gelu_and_slope(gu[rows, pl.ds(0, F)].astype(F32))
        gelu[...] = value
        hid_t[:, rows] = (value * gu[rows, pl.ds(F, F)].astype(F32)).astype(BF).T

    def compute_gates(k):
        half = lax.rem(k, 2)
        rows = pl.ds(pl.multiple_of(k * RC, RC), RC)
        row_copy(k, half).wait()
        d_hidden = dot_nt(dyr[half], wd[...])
        u = gu[rows, pl.ds(F, F)].astype(F32)
        gu[rows, pl.ds(0, F)] = ((d_hidden * u) * slope[...]).astype(BF)
        gu[rows, pl.ds(F, F)] = (d_hidden * gelu[...]).astype(BF)

        @pl.when(k + 2 < KC)
        def _():
            row_copy(k + 2, half).start()
            for cp in gate_copies(k + 2):
                cp.start()

    def compute_terms(k, part):
        rows = pl.ds(pl.multiple_of(k * RC, RC), RC)
        d_cat = gu[rows, :]
        if part == 0:
            cs[rows, :] = dot_nt(d_cat, wcat[pl.ds(other_col, HALF), :]).astype(BF)
        else:
            own[rows, :] = dot_nt(d_cat, wcat[pl.ds(own_col, HALF), :])

    def start_core(k):
        for i in range(PER):
            core_copy(k * PER + i).start()

    def compute_weights(j, part):
        half = lax.rem(j, 3)
        if part == 0:
            @pl.when(j + 2 < NB)
            def _():
                for which in range(2):
                    block_copy(which, j + 2, lax.rem(j + 2, 3)).start()

            block_copy(0, j, half).wait()
            rows = pl.ds(pl.multiple_of(j * CB, CB), CB)
            dw = dot_tn(xc[half], gu[...]).astype(BF)
            dwg[rows, :] = dw[:, :F]
            dwu[rows, :] = dw[:, F:]
        else:
            block_copy(1, j, half).wait()
            cols = pl.ds(pl.multiple_of(j * CB, CB), CB)
            dwd[:, cols] = jnp.dot(hid_t[...], dyc[half], preferred_element_type=F32).astype(BF)

    def when(condition, f, *args):
        @pl.when(condition)
        def _():
            f(*args)

    def send_terms(k):
        compute_terms(k, 0)
        start_core(k)

    def last_terms(k):
        compute_terms(k, 2)

        @pl.when(k + 1 < KC)
        def _():
            prepare(k + 1)

    def step(t, carry):
        k, odd = t // PER, lax.rem(t, PER) == 1
        first = t < K

        def stages(which):
            for stage in which:
                q = t - OFFS[stage]
                when((q >= 0) & (q < K), STAGES[stage], q)

        def slices(i):
            b = (t - K) * BPS + i
            for part in range(3):
                when((b >= 0) & (b < NSLICE) & (lax.rem(b, 3) == part), compute_weights, b // 3, part)

        when(first & jnp.logical_not(odd) & (k > 0), compute_gates, k)
        when(first & odd, compute_terms, k, 1)

        @pl.when(t == K - 2 * PER)
        def _():
            for which in range(2):
                block_copy(which, 0, 0).start()

        slices(0)
        stages((10, 9, 8, 7, 6))
        when(first & jnp.logical_not(odd) & (k > 0), send_terms, k)
        when(first & odd, last_terms, k)
        slices(1)
        stages((5, 4, 3, 2, 1))
        return carry

    LATE, EARLY = (10, 9, 8, 7, 6), (5, 4, 3, 2, 1)

    def stages(t, which, lo, hi):
        for stage in which:
            q = t - OFFS[stage]
            if hi - 1 - OFFS[stage] < 0 or lo - OFFS[stage] >= K:
                continue
            condition = None
            if lo < OFFS[stage]:
                condition = q >= 0
            if hi - 1 - OFFS[stage] >= K:
                condition = q < K if condition is None else condition & (q < K)
            if condition is None:
                STAGES[stage](q)
            else:
                when(condition, STAGES[stage], q)

    def chunk(k, more, lo, hi):
        t = PER * k
        compute_gates(k)
        stages(t, LATE, lo, hi)
        compute_terms(k, 0)
        start_core(k)
        stages(t, EARLY, lo, hi)
        stages(t + 1, LATE, lo, hi)
        compute_terms(k, 1)
        if more:
            prepare(k + 1)
        stages(t + 1, EARLY, lo, hi)

    def more_weights():
        w_copies[1].start()
        w_copies[2].start()

    prepare(0, more_weights)
    w_copies[0].wait()
    compute_gates(0)
    row_copy(1, 1).start()
    for cp in gate_copies(1):
        cp.start()
    w_copies[1].wait()
    w_copies[2].wait()
    compute_terms(0, 0)
    pl.semaphore_wait(barrier, len(partners))
    start_core(0)
    compute_terms(0, 1)
    prepare(1)
    stages(1, EARLY, 1, 2)

    def term_step(k, carry):
        chunk(k, True, PER, K - PER)
        return carry

    lax.fori_loop(1, KC - 1, term_step, 0)
    for j in range(2):
        for which in range(2):
            block_copy(which, j, j).start()
    chunk(jnp.int32(KC - 1), False, K - PER, K)

    def weight_step(i, carry):
        for n in range(2 * ST):
            for v in range(4):
                if v * 2 * ST // 4 == n:
                    compute_weights(2 * i + v // 2, v % 2)
            stages(K + ST * i + n // 2, (LATE, EARLY)[n % 2], K, MID)
        return carry

    lax.fori_loop(0, NB // 2, weight_step, 0)

    def tail_step(t, carry):
        stages(t, LATE + EARLY, MID, STEPS)
        return carry

    lax.fori_loop(MID, STEPS, tail_step, 0)

    def sent(ref, stage, color):
        pltpu.make_async_copy(ref, ref, ssem.at[stage, color]).wait()

    sent(cs, 0, 0)
    sent(cs, 9, 0)
    for e in range(2):
        for level, ref in enumerate((s1, s2, s3, s4), 1):
            sent(ref.at[e], level, e)
            sent(ref.at[e], 9 - level, e)


def write_out(*refs):
    sources, targets, sem = refs[:4], refs[4:8], refs[8]
    copies = [pltpu.make_async_copy(s, t, sem.at[i]) for i, (s, t) in enumerate(zip(sources, targets))]
    for cp in copies:
        cp.start()
    for cp in copies:
        cp.wait()


def solution(mesh):
    def step(x, dy, gate, up, w_gate, w_up, w_down):
        def out(*shape):
            return pltpu.VMEM(shape, BF)

        def buf(*shape, dtype=BF):
            return pltpu.VMEM(shape, dtype)

        scratch = [
            buf(F, D), buf(D, 2 * F), buf(ROWS, 2 * F), buf(RC, F, dtype=F32), buf(RC, F, dtype=F32), buf(F, ROWS),
            buf(2, RC, D), buf(3, ROWS, CB), buf(3, ROWS, CB),
            buf(ROWS, HALF, dtype=F32), buf(ROWS, HALF), buf(ROWS, HALF),
        ]
        for n, m in SZ[1:]:
            scratch += [buf(2, K * n, m), buf(2, K * n, m)]
        sem = pltpu.SemaphoreType.DMA
        scratch += [sem((10, 2)), sem((BASE[10],)), sem((3,)), sem((2, KC)), sem((2,)), sem((2, 3))]
        held = (
            pl.pallas_call(
                kernel,
                name="backward",
                out_shape=[out(ROWS, D), out(D, F), out(D, F), out(F, D)],
                in_specs=[pl.BlockSpec(memory_space=pl.ANY)] * 7,
                out_specs=[pl.BlockSpec(memory_space=pltpu.VMEM)] * 4,
                scratch_shapes=scratch,
                compiler_params=pltpu.CompilerParams(
                    collective_id=0, has_side_effects=True, vmem_limit_bytes=49 << 20
                ),
            )(x, dy, gate, up, w_gate, w_up, w_down)
        )
        return tuple(
            pl.pallas_call(
                write_out,
                name="write_out",
                out_shape=[jax.ShapeDtypeStruct(v.shape, BF) for v in held],
                in_specs=[pl.BlockSpec(memory_space=pltpu.VMEM)] * 4,
                out_specs=[pl.BlockSpec(memory_space=pl.ANY)] * 4,
                scratch_shapes=[sem((4,))],
                compiler_params=pltpu.CompilerParams(vmem_limit_bytes=1 << 20),
            )(*(pltpu.with_memory_space_constraint(v, pltpu.VMEM) for v in held))
        )

    tokens, columns, rows = P("dp", None), P(None, "tp"), P("tp", None)
    return jax.shard_map(
        step,
        mesh=mesh,
        in_specs=(tokens, tokens, P("dp", "tp"), P("dp", "tp"), columns, columns, rows),
        out_specs=(tokens, P("dp", "tp"), P("dp", "tp"), P(("dp", "tp"), None)),
        check_vma=False,
    )
```

```python
import functools

import jax
import jax.numpy as jnp
from jax import lax
from jax.experimental import pallas as pl
from jax.experimental.pallas import tpu as pltpu
from jax.sharding import PartitionSpec as P

MESH = pl.DeviceIdType.MESH
BF = jnp.bfloat16
F32 = jnp.float32

ROWS = 2048
D = 2048
F = 512
RC = 256
KC = ROWS // RC
K = 16
R = ROWS // K
PER = K // KC
HALF = D // 2
QC = HALF // 2
NB = 8
CB = D // NB

DELTAS = (1, 3, 3, 3, 3, 3, 3, 3, 4, 2)
OFFS = {i + 1: sum(DELTAS[: i + 1]) for i in range(10)}
LATE_CHUNKS = 4
EARLY_CHUNKS = 4
ST = 4
MID = K + ST * NB // 2
STEPS = max(MID, K + OFFS[10])
SLOTS = tuple(K if i in (2, 3, 6, 7) else min(K, 2 * d + (4 if i == 0 else 1)) for i, d in enumerate(DELTAS))
BASE = tuple(sum(SLOTS[:i]) for i in range(11))


def block_sizes():
    sizes = [(R, QC)]
    for _ in range(4):
        n, m = sizes[-1]
        sizes.append((n // 2, m) if n > 16 else (n, m // 2))
    return sizes


SZ = block_sizes()


C0 = 0.7978845608028654
C1 = 0.044715


def gelu_and_slope(g):
    square = g * g
    th = jnp.tanh(C0 * (g + C1 * (square * g)))
    cdf = 0.5 * (1.0 + th)
    slope = cdf + (g * (0.5 * (1.0 - th * th))) * (C0 * (1.0 + (3.0 * C1) * square))
    return g * cdf, slope


def dot_nt(a, b):
    return lax.dot_general(a, b, (((1,), (1,)), ((), ())), preferred_element_type=F32)


def dot_tn(a, b):
    return lax.dot_general(a, b, (((0,), (0,)), ((), ())), preferred_element_type=F32)


def kernel(
    x_hbm, dy_hbm, gate_hbm, up_hbm, wg_hbm, wu_hbm, wd_hbm,
    dx, dwg, dwu, dwd,
    wd, wcat, gu, gelu, slope, hid_t, dyr, xc, dyc, own, cs, cr,
    s1, r1, s2, r2, s3, r3, s4, r4,
    ssem, rsem, wsem, gsem, dsem, bsem,
):
    me = lax.axis_index("tp")
    c = lax.rem(me, 2)
    zl = lax.rem(me // 2, 2)
    zh = lax.rem(me // 4, 2)
    y = lax.rem(me // 8, 2)
    x = me // 16
    pc = me + 1 - 2 * c
    pz1 = me + 2 - 4 * zl
    pz2 = me + 4 - 8 * zh
    py = me + 8 - 16 * y
    px = me + 16 - 32 * x

    def row_copy(k, slot):
        return pltpu.make_async_copy(dy_hbm.at[pl.ds(k * RC, RC)], dyr.at[slot], dsem.at[slot])

    def gate_copies(k):
        rows = pl.ds(k * RC, RC)
        return (
            pltpu.make_async_copy(gate_hbm.at[rows], gu.at[rows, pl.ds(0, F)], gsem.at[0, k]),
            pltpu.make_async_copy(up_hbm.at[rows], gu.at[rows, pl.ds(F, F)], gsem.at[1, k]),
        )

    w_copies = (
        pltpu.make_async_copy(wd_hbm, wd, wsem.at[0]),
        pltpu.make_async_copy(wg_hbm, wcat.at[:, pl.ds(0, F)], wsem.at[1]),
        pltpu.make_async_copy(wu_hbm, wcat.at[:, pl.ds(F, F)], wsem.at[2]),
    )

    def block_copy(which, j, slot):
        columns = pl.ds(j * CB, CB)
        src, dst = ((x_hbm, xc), (dy_hbm, dyc))[which]
        return pltpu.make_async_copy(src.at[:, columns], dst.at[slot], bsem.at[which, slot])

    for cp in gate_copies(0):
        cp.start()
    row_copy(0, 0).start()
    w_copies[0].start()

    barrier = pltpu.get_barrier_semaphore()
    partners = (pc, pz1, pz2, py, px)
    for p in partners:
        pl.semaphore_signal(barrier, inc=1, device_id=(0, p), device_id_type=MESH)

    def remote(src, dst, stage, color, k, p):
        return pltpu.make_async_remote_copy(
            src_ref=src, dst_ref=dst,
            send_sem=ssem.at[stage, color], recv_sem=rsem.at[slot(stage, k)],
            device_id=(0, p), device_id_type=MESH,
        )

    def m16(v):
        return pl.multiple_of(v, 16)

    own_col = pl.multiple_of(c * HALF, HALF)
    other_col = pl.multiple_of((1 - c) * HALF, HALF)

    def route(e, k):
        a, b, pa, pb = ((x, y, px, py), (y, x, py, px))[e]
        late = (k >= K - LATE_CHUNKS).astype(jnp.int32)
        swap, pswap = late * (b - zl), late * (pb - pz1)
        return (a, zl + swap, b - swap, zh), (pa, pz1 + pswap, pb - pswap, pz2)

    def slot(stage, k):
        return BASE[stage] + lax.rem(k, SLOTS[stage])

    def core_copy(k):
        rows = pl.ds(pl.multiple_of(k * R, R), R)
        return remote(cs.at[rows], cr.at[rows], 0, 0, k, pc)

    def m128(v):
        return v if isinstance(v, int) else pl.multiple_of(v, 128)

    def level_copy(level, e, k):
        s, r = ((s1, r1), (s2, r2), (s3, r3), (s4, r4))[level - 1]
        p = route(e, k)[1][level - 1]
        n = SZ[level][0]
        rows = pl.ds(m16(k * n), n)
        return remote(s.at[e, rows], r.at[e, rows], level, e, k, p)

    def received(stage, k):
        level = stage if stage < 5 else 9 - stage
        if level == 0:
            ref = cr.at[pl.ds(m16(k * R), R)]
        else:
            n = SZ[level][0]
            ref = (r1, r2, r3, r4)[level - 1].at[:, pl.ds(m16(k * n), n)]
        pltpu.make_async_copy(ref, ref, rsem.at[slot(stage, k)]).wait()

    def offset(level, e, k, flip=False):
        bits = route(e, k)[0]
        row = col = 0
        for i in range(level):
            b = bits[i]
            if flip and i == level - 1:
                b = 1 - b
            if SZ[i + 1][0] < SZ[i][0]:
                row = row + b * SZ[i + 1][0]
            else:
                col = col + b * SZ[i + 1][1]
        return row, col

    def gather_copies(level, e, k):
        bits, p = route(e, k)
        crossed = ((k < EARLY_CHUNKS) | (k >= K - LATE_CHUNKS)).astype(jnp.int32)
        n, m = SZ[level]
        row, col = offset(level, e, k)
        p = p[level - 1] if level in (1, 4) else p[level - 1] + crossed * (p[4 - level] - p[level - 1])
        cols = pl.ds(pl.multiple_of(own_col + e * QC + col, 128), m)
        rows = [pl.ds(m16(k * R + row), n)]
        if level == 2:
            half = n // 2
            first = row + crossed * (offset(1, e, k)[0] + bits[2] * half - row)
            stride = half + crossed * (n - half)
            rows = [pl.ds(m16(k * R + first), half), pl.ds(m16(k * R + first + stride), half)]
        return [remote(dx.at[r, cols], dx.at[r, cols], 9 - level, e, k, p) for r in rows]

    def out_copy(k):
        view = dx.at[pl.ds(pl.multiple_of(k * R, R), R), pl.ds(own_col, HALF)]
        return remote(view, view, 9, 0, k, pc)

    def total(level, e, k, off, size):
        (row, col), (n, m) = off, size
        rows, cols = pl.ds(m16(k * R + row), n), pl.ds(m128(e * QC + col), m)
        acc = own[rows, cols] + cr[rows, cols].astype(F32)
        recv = (r1, r2, r3, r4)
        for i in range(level):
            krow, kcol = offset(i + 1, e, k)
            rows = pl.ds(m16(k * SZ[i + 1][0] + row - krow), n)
            acc = acc + recv[i][e, rows, pl.ds(m128(col - kcol), m)].astype(F32)
        return acc

    def reduce_stage(level, k):
        received(level - 1, k)
        for e in range(2):
            n = SZ[level][0]
            stage = (s1, s2, s3, s4)[level - 1]
            stage[e, pl.ds(m16(k * n), n), :] = total(level - 1, e, k, offset(level, e, k, True), SZ[level]).astype(BF)
            level_copy(level, e, k).start()

    def finish_stage(k):
        n, m = SZ[4]
        received(4, k)
        for e in range(2):
            row, col = offset(4, e, k)
            cols = pl.ds(pl.multiple_of(own_col + e * QC + col, 128), m)
            dx[pl.ds(m16(k * R + row), n), cols] = total(4, e, k, (row, col), (n, m)).astype(BF)
            for cp in gather_copies(4, e, k):
                cp.start()

    def gather_stage(level, k):
        received(8 - level, k)
        for e in range(2):
            for cp in gather_copies(level, e, k):
                cp.start()

    def last_stage(k):
        received(8, k)
        out_copy(k).start()

    STAGES = {
        1: lambda k: reduce_stage(1, k),
        2: lambda k: reduce_stage(2, k),
        3: lambda k: reduce_stage(3, k),
        4: lambda k: reduce_stage(4, k),
        5: finish_stage,
        6: lambda k: gather_stage(3, k),
        7: lambda k: gather_stage(2, k),
        8: lambda k: gather_stage(1, k),
        9: last_stage,
        10: lambda k: received(9, k),
    }

    def prepare(k, then=None):
        rows = pl.ds(pl.multiple_of(k * RC, RC), RC)
        for cp in gate_copies(k):
            cp.wait()
        if then is not None:
            then()
        value, slope[...] = gelu_and_slope(gu[rows, pl.ds(0, F)].astype(F32))
        gelu[...] = value
        hid_t[:, rows] = (value * gu[rows, pl.ds(F, F)].astype(F32)).astype(BF).T

    def compute_gates(k):
        half = lax.rem(k, 2)
        rows = pl.ds(pl.multiple_of(k * RC, RC), RC)
        row_copy(k, half).wait()
        d_hidden = dot_nt(dyr[half], wd[...])
        u = gu[rows, pl.ds(F, F)].astype(F32)
        gu[rows, pl.ds(0, F)] = ((d_hidden * u) * slope[...]).astype(BF)
        gu[rows, pl.ds(F, F)] = (d_hidden * gelu[...]).astype(BF)

        @pl.when(k + 2 < KC)
        def _():
            row_copy(k + 2, half).start()
            for cp in gate_copies(k + 2):
                cp.start()

    def compute_terms(k, part):
        rows = pl.ds(pl.multiple_of(k * RC, RC), RC)
        d_cat = gu[rows, :]
        if part == 0:
            cs[rows, :] = dot_nt(d_cat, wcat[pl.ds(other_col, HALF), :]).astype(BF)
        else:
            own[rows, :] = dot_nt(d_cat, wcat[pl.ds(own_col, HALF), :])

    def start_core(k):
        for i in range(PER):
            core_copy(k * PER + i).start()

    def compute_weights(j, part):
        half = lax.rem(j, 3)
        if part == 0:
            @pl.when(j + 2 < NB)
            def _():
                for which in range(2):
                    block_copy(which, j + 2, lax.rem(j + 2, 3)).start()

            block_copy(0, j, half).wait()
            rows = pl.ds(pl.multiple_of(j * CB, CB), CB)
            dw = dot_tn(xc[half], gu[...]).astype(BF)
            dwg[rows, :] = dw[:, :F]
            dwu[rows, :] = dw[:, F:]
        else:
            block_copy(1, j, half).wait()
            cols = pl.ds(pl.multiple_of(j * CB, CB), CB)
            dwd[:, cols] = jnp.dot(hid_t[...], dyc[half], preferred_element_type=F32).astype(BF)

    def when(condition, f, *args):
        @pl.when(condition)
        def _():
            f(*args)

    def send_terms(k):
        compute_terms(k, 0)
        start_core(k)

    def last_terms(k):
        compute_terms(k, 2)

        @pl.when(k + 1 < KC)
        def _():
            prepare(k + 1)

    def step(t, carry):
        k, odd = t // PER, lax.rem(t, PER) == 1
        first = t < K

        def stages(which):
            for stage in which:
                q = t - OFFS[stage]
                when((q >= 0) & (q < K), STAGES[stage], q)

        def slices(i):
            b = (t - K) * BPS + i
            for part in range(3):
                when((b >= 0) & (b < NSLICE) & (lax.rem(b, 3) == part), compute_weights, b // 3, part)

        when(first & jnp.logical_not(odd) & (k > 0), compute_gates, k)
        when(first & odd, compute_terms, k, 1)

        @pl.when(t == K - 2 * PER)
        def _():
            for which in range(2):
                block_copy(which, 0, 0).start()

        slices(0)
        stages((10, 9, 8, 7, 6))
        when(first & jnp.logical_not(odd) & (k > 0), send_terms, k)
        when(first & odd, last_terms, k)
        slices(1)
        stages((5, 4, 3, 2, 1))
        return carry

    LATE, EARLY = (10, 9, 8, 7, 6), (5, 4, 3, 2, 1)

    def stages(t, which, lo, hi):
        for stage in which:
            q = t - OFFS[stage]
            if hi - 1 - OFFS[stage] < 0 or lo - OFFS[stage] >= K:
                continue
            condition = None
            if lo < OFFS[stage]:
                condition = q >= 0
            if hi - 1 - OFFS[stage] >= K:
                condition = q < K if condition is None else condition & (q < K)
            if condition is None:
                STAGES[stage](q)
            else:
                when(condition, STAGES[stage], q)

    def chunk(k, more, lo, hi):
        t = PER * k
        compute_gates(k)
        stages(t, LATE, lo, hi)
        compute_terms(k, 0)
        start_core(k)
        stages(t, EARLY, lo, hi)
        stages(t + 1, LATE, lo, hi)
        compute_terms(k, 1)
        if more:
            prepare(k + 1)
        stages(t + 1, EARLY, lo, hi)

    def more_weights():
        w_copies[1].start()
        w_copies[2].start()

    prepare(0, more_weights)
    w_copies[0].wait()
    compute_gates(0)
    row_copy(1, 1).start()
    for cp in gate_copies(1):
        cp.start()
    w_copies[1].wait()
    w_copies[2].wait()
    compute_terms(0, 0)
    pl.semaphore_wait(barrier, len(partners))
    start_core(0)
    compute_terms(0, 1)
    prepare(1)
    stages(jnp.int32(1), EARLY, 1, 2)

    def term_step(k, carry):
        chunk(k, True, PER, K - PER)
        return carry

    lax.fori_loop(1, KC - 1, term_step, 0)
    for j in range(2):
        for which in range(2):
            block_copy(which, j, j).start()
    chunk(jnp.int32(KC - 1), False, K - PER, K)

    def weight_step(i, carry):
        for n in range(2 * ST):
            for v in range(4):
                if v * 2 * ST // 4 == n:
                    compute_weights(2 * i + v // 2, v % 2)
            stages(K + ST * i + n // 2, (LATE, EARLY)[n % 2], K, MID)
        return carry

    lax.fori_loop(0, NB // 2, weight_step, 0)

    def tail_step(t, carry):
        stages(t, LATE + EARLY, MID, STEPS)
        return carry

    lax.fori_loop(MID, STEPS, tail_step, 0)

    def sent(ref, stage, color):
        pltpu.make_async_copy(ref, ref, ssem.at[stage, color]).wait()

    sent(cs, 0, 0)
    sent(cs, 9, 0)
    for e in range(2):
        for level, ref in enumerate((s1, s2, s3, s4), 1):
            sent(ref.at[e], level, e)
            sent(ref.at[e], 9 - level, e)


def write_out(*refs):
    sources, targets, sem = refs[:4], refs[4:8], refs[8]
    copies = [pltpu.make_async_copy(s, t, sem.at[i]) for i, (s, t) in enumerate(zip(sources, targets))]
    for cp in copies:
        cp.start()
    for cp in copies:
        cp.wait()


def solution(mesh):
    def step(x, dy, gate, up, w_gate, w_up, w_down):
        def out(*shape):
            return pltpu.VMEM(shape, BF)

        def buf(*shape, dtype=BF):
            return pltpu.VMEM(shape, dtype)

        scratch = [
            buf(F, D), buf(D, 2 * F), buf(ROWS, 2 * F), buf(RC, F, dtype=F32), buf(RC, F, dtype=F32), buf(F, ROWS),
            buf(2, RC, D), buf(3, ROWS, CB), buf(3, ROWS, CB),
            buf(ROWS, HALF, dtype=F32), buf(ROWS, HALF), buf(ROWS, HALF),
        ]
        for n, m in SZ[1:]:
            scratch += [buf(2, K * n, m), buf(2, K * n, m)]
        sem = pltpu.SemaphoreType.DMA
        scratch += [sem((10, 2)), sem((BASE[10],)), sem((3,)), sem((2, KC)), sem((2,)), sem((2, 3))]
        held = (
            pl.pallas_call(
                kernel,
                name="backward",
                out_shape=[out(ROWS, D), out(D, F), out(D, F), out(F, D)],
                in_specs=[pl.BlockSpec(memory_space=pl.ANY)] * 7,
                out_specs=[pl.BlockSpec(memory_space=pltpu.VMEM)] * 4,
                scratch_shapes=scratch,
                compiler_params=pltpu.CompilerParams(
                    collective_id=0, has_side_effects=True, vmem_limit_bytes=49 << 20
                ),
            )(x, dy, gate, up, w_gate, w_up, w_down)
        )
        return tuple(
            pl.pallas_call(
                write_out,
                name="write_out",
                out_shape=[jax.ShapeDtypeStruct(v.shape, BF) for v in held],
                in_specs=[pl.BlockSpec(memory_space=pltpu.VMEM)] * 4,
                out_specs=[pl.BlockSpec(memory_space=pl.ANY)] * 4,
                scratch_shapes=[sem((4,))],
                compiler_params=pltpu.CompilerParams(vmem_limit_bytes=1 << 20),
            )(*(pltpu.with_memory_space_constraint(v, pltpu.VMEM) for v in held))
        )

    tokens, columns, rows = P("dp", None), P(None, "tp"), P("tp", None)
    return jax.shard_map(
        step,
        mesh=mesh,
        in_specs=(tokens, tokens, P("dp", "tp"), P("dp", "tp"), columns, columns, rows),
        out_specs=(tokens, P("dp", "tp"), P("dp", "tp"), P(("dp", "tp"), None)),
        check_vma=False,
    )
```

```python
import functools

import jax
import jax.numpy as jnp
from jax import lax
from jax.experimental import pallas as pl
from jax.experimental.pallas import tpu as pltpu
from jax.sharding import PartitionSpec as P

MESH = pl.DeviceIdType.MESH
BF = jnp.bfloat16
F32 = jnp.float32

ROWS = 2048
D = 2048
F = 512
RC = 256
KC = ROWS // RC
K = 16
R = ROWS // K
PER = K // KC
HALF = D // 2
QC = HALF // 2
NB = 8
CB = D // NB

DELTAS = (1, 3, 3, 3, 3, 3, 3, 4, 4, 2)
OFFS = {i + 1: sum(DELTAS[: i + 1]) for i in range(10)}
LATE_CHUNKS = 4
EARLY_CHUNKS = 4
ST = 4
MID = K + ST * NB // 2
STEPS = max(MID, K + OFFS[10])
SLOTS = tuple(K if i in (2, 3, 6, 7) else min(K, 2 * d + (4 if i == 0 else 1)) for i, d in enumerate(DELTAS))
BASE = tuple(sum(SLOTS[:i]) for i in range(11))


def block_sizes():
    sizes = [(R, QC)]
    for _ in range(4):
        n, m = sizes[-1]
        sizes.append((n // 2, m) if n > 16 else (n, m // 2))
    return sizes


SZ = block_sizes()


C0 = 0.7978845608028654
C1 = 0.044715


def gelu_and_slope(g):
    square = g * g
    th = jnp.tanh(C0 * (g + C1 * (square * g)))
    cdf = 0.5 * (1.0 + th)
    slope = cdf + (g * (0.5 * (1.0 - th * th))) * (C0 * (1.0 + (3.0 * C1) * square))
    return g * cdf, slope


def dot_nt(a, b):
    return lax.dot_general(a, b, (((1,), (1,)), ((), ())), preferred_element_type=F32)


def dot_tn(a, b):
    return lax.dot_general(a, b, (((0,), (0,)), ((), ())), preferred_element_type=F32)


def kernel(
    x_hbm, dy_hbm, gate_hbm, up_hbm, wg_hbm, wu_hbm, wd_hbm,
    dx, dwg, dwu, dwd,
    wd, wcat, gu, gelu, slope, hid_t, dyr, xc, dyc, own, cs, cr,
    s1, r1, s2, r2, s3, r3, s4, r4,
    ssem, rsem, wsem, gsem, dsem, bsem,
):
    me = lax.axis_index("tp")
    c = lax.rem(me, 2)
    zl = lax.rem(me // 2, 2)
    zh = lax.rem(me // 4, 2)
    y = lax.rem(me // 8, 2)
    x = me // 16
    pc = me + 1 - 2 * c
    pz1 = me + 2 - 4 * zl
    pz2 = me + 4 - 8 * zh
    py = me + 8 - 16 * y
    px = me + 16 - 32 * x

    def row_copy(k, slot):
        return pltpu.make_async_copy(dy_hbm.at[pl.ds(k * RC, RC)], dyr.at[slot], dsem.at[slot])

    def gate_copies(k):
        rows = pl.ds(k * RC, RC)
        return (
            pltpu.make_async_copy(gate_hbm.at[rows], gu.at[rows, pl.ds(0, F)], gsem.at[0, k % 2 if isinstance(k, int) else lax.rem(k, 2)]),
            pltpu.make_async_copy(up_hbm.at[rows], gu.at[rows, pl.ds(F, F)], gsem.at[1, k % 2 if isinstance(k, int) else lax.rem(k, 2)]),
        )

    w_copies = (
        pltpu.make_async_copy(wd_hbm, wd, wsem.at[0]),
        pltpu.make_async_copy(wg_hbm, wcat.at[:, pl.ds(0, F)], wsem.at[1]),
        pltpu.make_async_copy(wu_hbm, wcat.at[:, pl.ds(F, F)], wsem.at[2]),
    )

    def block_copy(which, j, slot):
        columns = pl.ds(j * CB, CB)
        src, dst = ((x_hbm, xc), (dy_hbm, dyc))[which]
        return pltpu.make_async_copy(src.at[:, columns], dst.at[slot], bsem.at[which, slot])

    for cp in gate_copies(0):
        cp.start()
    row_copy(0, 0).start()
    w_copies[0].start()

    barrier = pltpu.get_barrier_semaphore()
    partners = (pc, pz1, pz2, py, px)
    for p in partners:
        pl.semaphore_signal(barrier, inc=1, device_id=(0, p), device_id_type=MESH)

    def remote(src, dst, stage, color, k, p):
        return pltpu.make_async_remote_copy(
            src_ref=src, dst_ref=dst,
            send_sem=ssem.at[stage, color], recv_sem=rsem.at[slot(stage, k)],
            device_id=(0, p), device_id_type=MESH,
        )

    def m16(v):
        return pl.multiple_of(v, 16)

    own_col = pl.multiple_of(c * HALF, HALF)
    other_col = pl.multiple_of((1 - c) * HALF, HALF)

    def route(e, k):
        a, b, pa, pb = ((x, y, px, py), (y, x, py, px))[e]
        late = (k >= K - LATE_CHUNKS).astype(jnp.int32)
        swap, pswap = late * (b - zl), late * (pb - pz1)
        return (a, zl + swap, b - swap, zh), (pa, pz1 + pswap, pb - pswap, pz2)

    def slot(stage, k):
        return BASE[stage] + lax.rem(k, SLOTS[stage])

    def core_copy(k):
        rows = pl.ds(pl.multiple_of(k * R, R), R)
        return remote(cs.at[rows], cr.at[rows], 0, 0, k, pc)

    def m128(v):
        return v if isinstance(v, int) else pl.multiple_of(v, 128)

    def level_copy(level, e, k):
        s, r = ((s1, r1), (s2, r2), (s3, r3), (s4, r4))[level - 1]
        p = route(e, k)[1][level - 1]
        n = SZ[level][0]
        rows = pl.ds(m16(k * n), n)
        return remote(s.at[e, rows], r.at[e, rows], level, e, k, p)

    def received(stage, k):
        level = stage if stage < 5 else 9 - stage
        if level == 0:
            ref = cr.at[pl.ds(m16(k * R), R)]
        else:
            n = SZ[level][0]
            ref = (r1, r2, r3, r4)[level - 1].at[:, pl.ds(m16(k * n), n)]
        pltpu.make_async_copy(ref, ref, rsem.at[slot(stage, k)]).wait()

    def offset(level, e, k, flip=False):
        bits = route(e, k)[0]
        row = col = 0
        for i in range(level):
            b = bits[i]
            if flip and i == level - 1:
                b = 1 - b
            if SZ[i + 1][0] < SZ[i][0]:
                row = row + b * SZ[i + 1][0]
            else:
                col = col + b * SZ[i + 1][1]
        return row, col

    def gather_copies(level, e, k):
        bits, p = route(e, k)
        crossed = ((k < EARLY_CHUNKS) | (k >= K - LATE_CHUNKS)).astype(jnp.int32)
        n, m = SZ[level]
        row, col = offset(level, e, k)
        p = p[level - 1] if level in (1, 4) else p[level - 1] + crossed * (p[4 - level] - p[level - 1])
        cols = pl.ds(pl.multiple_of(own_col + e * QC + col, 128), m)
        rows = [pl.ds(m16(k * R + row), n)]
        if level == 2:
            half = n // 2
            first = row + crossed * (offset(1, e, k)[0] + bits[2] * half - row)
            stride = half + crossed * (n - half)
            rows = [pl.ds(m16(k * R + first), half), pl.ds(m16(k * R + first + stride), half)]
        return [remote(dx.at[r, cols], dx.at[r, cols], 9 - level, e, k, p) for r in rows]

    def out_copy(k):
        view = dx.at[pl.ds(pl.multiple_of(k * R, R), R), pl.ds(own_col, HALF)]
        return remote(view, view, 9, 0, k, pc)

    def total(level, e, k, off, size):
        (row, col), (n, m) = off, size
        rows, cols = pl.ds(m16(k * R + row), n), pl.ds(m128(e * QC + col), m)
        acc = own[rows, cols] + cr[rows, cols].astype(F32)
        recv = (r1, r2, r3, r4)
        for i in range(level):
            krow, kcol = offset(i + 1, e, k)
            rows = pl.ds(m16(k * SZ[i + 1][0] + row - krow), n)
            acc = acc + recv[i][e, rows, pl.ds(m128(col - kcol), m)].astype(F32)
        return acc

    def reduce_stage(level, k):
        received(level - 1, k)
        for e in range(2):
            n = SZ[level][0]
            stage = (s1, s2, s3, s4)[level - 1]
            stage[e, pl.ds(m16(k * n), n), :] = total(level - 1, e, k, offset(level, e, k, True), SZ[level]).astype(BF)
            level_copy(level, e, k).start()

    def finish_stage(k):
        n, m = SZ[4]
        received(4, k)
        for e in range(2):
            row, col = offset(4, e, k)
            cols = pl.ds(pl.multiple_of(own_col + e * QC + col, 128), m)
            dx[pl.ds(m16(k * R + row), n), cols] = total(4, e, k, (row, col), (n, m)).astype(BF)
            for cp in gather_copies(4, e, k):
                cp.start()

    def gather_stage(level, k):
        received(8 - level, k)
        for e in range(2):
            for cp in gather_copies(level, e, k):
                cp.start()

    def last_stage(k):
        received(8, k)
        out_copy(k).start()

    STAGES = {
        1: lambda k: reduce_stage(1, k),
        2: lambda k: reduce_stage(2, k),
        3: lambda k: reduce_stage(3, k),
        4: lambda k: reduce_stage(4, k),
        5: finish_stage,
        6: lambda k: gather_stage(3, k),
        7: lambda k: gather_stage(2, k),
        8: lambda k: gather_stage(1, k),
        9: last_stage,
        10: lambda k: received(9, k),
    }

    def prepare(k, then=None):
        rows = pl.ds(pl.multiple_of(k * RC, RC), RC)
        for cp in gate_copies(k):
            cp.wait()
        if then is not None:
            then()
        value, slope[...] = gelu_and_slope(gu[rows, pl.ds(0, F)].astype(F32))
        gelu[...] = value
        hid_t[:, rows] = (value * gu[rows, pl.ds(F, F)].astype(F32)).astype(BF).T

    def compute_gates(k):
        half = lax.rem(k, 2)
        rows = pl.ds(pl.multiple_of(k * RC, RC), RC)
        row_copy(k, half).wait()
        d_hidden = dot_nt(dyr[half], wd[...])
        u = gu[rows, pl.ds(F, F)].astype(F32)
        gu[rows, pl.ds(0, F)] = ((d_hidden * u) * slope[...]).astype(BF)
        gu[rows, pl.ds(F, F)] = (d_hidden * gelu[...]).astype(BF)

        @pl.when(k + 2 < KC)
        def _():
            row_copy(k + 2, half).start()
            for cp in gate_copies(k + 2):
                cp.start()

    def compute_terms(k, part):
        rows = pl.ds(pl.multiple_of(k * RC, RC), RC)
        d_cat = gu[rows, :]
        if part == 0:
            cs[rows, :] = dot_nt(d_cat, wcat[pl.ds(other_col, HALF), :]).astype(BF)
        else:
            own[rows, :] = dot_nt(d_cat, wcat[pl.ds(own_col, HALF), :])

    def start_core(k):
        for i in range(PER):
            core_copy(k * PER + i).start()

    def compute_weights(j, part):
        half = lax.rem(j, 3)
        if part == 0:
            @pl.when(j + 2 < NB)
            def _():
                for which in range(2):
                    block_copy(which, j + 2, lax.rem(j + 2, 3)).start()

            block_copy(0, j, half).wait()
            rows = pl.ds(pl.multiple_of(j * CB, CB), CB)
            dw = dot_tn(xc[half], gu[...]).astype(BF)
            dwg[rows, :] = dw[:, :F]
            dwu[rows, :] = dw[:, F:]
        else:
            block_copy(1, j, half).wait()
            cols = pl.ds(pl.multiple_of(j * CB, CB), CB)
            dwd[:, cols] = jnp.dot(hid_t[...], dyc[half], preferred_element_type=F32).astype(BF)

    def when(condition, f, *args):
        @pl.when(condition)
        def _():
            f(*args)

    def send_terms(k):
        compute_terms(k, 0)
        start_core(k)

    def last_terms(k):
        compute_terms(k, 2)

        @pl.when(k + 1 < KC)
        def _():
            prepare(k + 1)

    def step(t, carry):
        k, odd = t // PER, lax.rem(t, PER) == 1
        first = t < K

        def stages(which):
            for stage in which:
                q = t - OFFS[stage]
                when((q >= 0) & (q < K), STAGES[stage], q)

        def slices(i):
            b = (t - K) * BPS + i
            for part in range(3):
                when((b >= 0) & (b < NSLICE) & (lax.rem(b, 3) == part), compute_weights, b // 3, part)

        when(first & jnp.logical_not(odd) & (k > 0), compute_gates, k)
        when(first & odd, compute_terms, k, 1)

        @pl.when(t == K - 2 * PER)
        def _():
            for which in range(2):
                block_copy(which, 0, 0).start()

        slices(0)
        stages((10, 9, 8, 7, 6))
        when(first & jnp.logical_not(odd) & (k > 0), send_terms, k)
        when(first & odd, last_terms, k)
        slices(1)
        stages((5, 4, 3, 2, 1))
        return carry

    LATE, EARLY = (10, 9, 8, 7, 6), (5, 4, 3, 2, 1)

    def stages(t, which, lo, hi):
        for stage in which:
            q = t - OFFS[stage]
            if hi - 1 - OFFS[stage] < 0 or lo - OFFS[stage] >= K:
                continue
            condition = None
            if lo < OFFS[stage]:
                condition = q >= 0
            if hi - 1 - OFFS[stage] >= K:
                condition = q < K if condition is None else condition & (q < K)
            if condition is None:
                STAGES[stage](q)
            else:
                when(condition, STAGES[stage], q)

    def chunk(k, more, lo, hi):
        t = PER * k
        compute_gates(k)
        stages(t, LATE, lo, hi)
        compute_terms(k, 0)
        start_core(k)
        stages(t, EARLY, lo, hi)
        stages(t + 1, LATE, lo, hi)
        compute_terms(k, 1)
        if more:
            prepare(k + 1)
        stages(t + 1, EARLY, lo, hi)

    def more_weights():
        w_copies[1].start()
        w_copies[2].start()

    prepare(0, more_weights)
    w_copies[0].wait()
    compute_gates(0)
    row_copy(1, 1).start()
    for cp in gate_copies(1):
        cp.start()
    w_copies[1].wait()
    w_copies[2].wait()
    compute_terms(0, 0)
    pl.semaphore_wait(barrier, len(partners))
    start_core(0)
    compute_terms(0, 1)
    prepare(1)
    stages(jnp.int32(1), EARLY, 1, 2)

    def term_step(k, carry):
        chunk(k, True, PER, K - PER)
        return carry

    lax.fori_loop(1, KC - 1, term_step, 0)
    for j in range(2):
        for which in range(2):
            block_copy(which, j, j).start()
    chunk(jnp.int32(KC - 1), False, K - PER, K)

    def weight_step(j, carry):
        for n in range(ST):
            if n == 0:
                compute_weights(j, 0)
            if n == ST // 2:
                compute_weights(j, 1)
            stages(K + (ST // 2) * j + n // 2, (LATE, EARLY)[n % 2], K, MID)
        return carry

    lax.fori_loop(0, NB, weight_step, 0)

    def tail_step(t, carry):
        stages(t, LATE + EARLY, MID, STEPS)
        return carry

    lax.fori_loop(MID, STEPS, tail_step, 0)

    def sent(ref, stage, color):
        pltpu.make_async_copy(ref, ref, ssem.at[stage, color]).wait()

    sent(cs, 0, 0)
    sent(cs, 9, 0)
    for e in range(2):
        for level, ref in enumerate((s1, s2, s3, s4), 1):
            sent(ref.at[e], level, e)
            sent(ref.at[e], 9 - level, e)


def write_out(*refs):
    sources, targets, sem = refs[:4], refs[4:8], refs[8]
    copies = []
    for s, t in zip(sources, targets):
        n = s.shape[0] // 4
        for i in range(4):
            copies.append(pltpu.make_async_copy(s.at[pl.ds(i * n, n)], t.at[pl.ds(i * n, n)], sem.at[len(copies)]))
    for cp in copies:
        cp.start()
    for cp in copies:
        cp.wait()


def solution(mesh):
    def step(x, dy, gate, up, w_gate, w_up, w_down):
        def out(*shape):
            return pltpu.VMEM(shape, BF)

        def buf(*shape, dtype=BF):
            return pltpu.VMEM(shape, dtype)

        scratch = [
            buf(F, D), buf(D, 2 * F), buf(ROWS, 2 * F), buf(RC, F, dtype=F32), buf(RC, F, dtype=F32), buf(F, ROWS),
            buf(2, RC, D), buf(3, ROWS, CB), buf(3, ROWS, CB),
            buf(ROWS, HALF, dtype=F32), buf(ROWS, HALF), buf(ROWS, HALF),
        ]
        for n, m in SZ[1:]:
            scratch += [buf(2, K * n, m), buf(2, K * n, m)]
        sem = pltpu.SemaphoreType.DMA
        scratch += [sem((10, 2)), sem((BASE[10],)), sem((3,)), sem((2, 2)), sem((2,)), sem((2, 3))]
        held = (
            pl.pallas_call(
                kernel,
                name="backward",
                out_shape=[out(ROWS, D), out(D, F), out(D, F), out(F, D)],
                in_specs=[pl.BlockSpec(memory_space=pl.ANY)] * 7,
                out_specs=[pl.BlockSpec(memory_space=pltpu.VMEM)] * 4,
                scratch_shapes=scratch,
                compiler_params=pltpu.CompilerParams(
                    collective_id=0, has_side_effects=True, vmem_limit_bytes=49 << 20
                ),
            )(x, dy, gate, up, w_gate, w_up, w_down)
        )
        return tuple(
            pl.pallas_call(
                write_out,
                name="write_out",
                out_shape=[jax.ShapeDtypeStruct(v.shape, BF) for v in held],
                in_specs=[pl.BlockSpec(memory_space=pltpu.VMEM)] * 4,
                out_specs=[pl.BlockSpec(memory_space=pl.ANY)] * 4,
                scratch_shapes=[sem((16,))],
                compiler_params=pltpu.CompilerParams(vmem_limit_bytes=1 << 20),
            )(*(pltpu.with_memory_space_constraint(v, pltpu.VMEM) for v in held))
        )

    tokens, columns, rows = P("dp", None), P(None, "tp"), P("tp", None)
    return jax.shard_map(
        step,
        mesh=mesh,
        in_specs=(tokens, tokens, P("dp", "tp"), P("dp", "tp"), columns, columns, rows),
        out_specs=(tokens, P("dp", "tp"), P("dp", "tp"), P(("dp", "tp"), None)),
        check_vma=False,
    )
```
